32 devices in a mesh: row: 16 (over z, y, x), col: 2 (over core).
Axes of the slice: x: 2, y: 2, z: 4, core: 2. Of those that a mesh axis runs over, the one named last changes fastest.
Arguments:
- tokens: bfloat16 [256, 8192], P('row', 'col'), may hold values from -6 to 6
- norm_gain: float32 [8192], P('col'), may hold values from 0.1 to 1.9
- gate_weight: bfloat16 [8192, 28672], P('col', 'row'), may hold values from -0.0625 to 0.0625
- up_weight: bfloat16 [8192, 28672], P('col', 'row'), may hold values from -0.0625 to 0.0625
- down_weight: bfloat16 [28672, 8192], P('row', 'col'), may hold values from -0.03125 to 0.03125
Outputs:
- mixed: bfloat16 [256, 8192], P('row', 'col')
The draws below stay inside these ranges and needn't reach their ends.
All inputs are finite; a program needn't handle non-finite values.
Results may differ from the reference program's by a relative error of at most 0.0065.
Values may be sent and summed in bfloat16 or wider, within the bound.
No kernel may reach another device: no remote copies, remote signals or barrier semaphores. Data moves between devices by JAX's collectives and lax.ppermute only.
A program may use at most 128 MiB of HBM per device.

```python
import jax
import jax.numpy as jnp
from jax import lax

D = 8192
FF = 28672
TOKENS = 256


def block_levels(rng, dims, shards, smallest, largest):
    def one(position, parts):
        heights = jax.random.uniform(jax.random.fold_in(jax.random.fold_in(rng, 6), position), (parts,), jnp.float32, smallest / len(shards), largest / len(shards))
        return jnp.repeat(jnp.exp(heights), dims[position] // parts).reshape((-1,) + (1,) * (len(dims) - position - 1))

    level = one(*shards[0])
    for cut in shards[1:]:
        level = level * one(*cut)
    return level


def centred(stream_key, extent, deviation, reach, cuts=(), held_as=jnp.bfloat16):
    array = jax.random.normal(stream_key, extent, jnp.float32) * deviation
    if len(cuts) > 0:
        array = block_levels(stream_key, extent, cuts, -0.22, 0.18) * array
    return jnp.clip(array, min=-reach, max=reach).astype(held_as)


def setup_inputs(seed: int = 0) -> dict:
    seeds = jax.random.split(jax.random.key(seed), 6)
    tokens = centred(seeds[0], (TOKENS, D), 1.0, 6.0, ((0, 16), (1, 2)))
    norm_gain = jnp.clip(1.0 + 0.18 * jax.random.normal(seeds[1], (D,), jnp.float32), 0.1, 1.9)
    gate_weight = centred(seeds[2], (D, FF), D ** -0.5, 0.0625, ((0, 2), (1, 16)))
    up_weight = centred(seeds[3], (D, FF), D ** -0.5, 0.0625, ((0, 2), (1, 16)))
    down_weight = centred(seeds[4], (FF, D), FF ** -0.5, 0.03125, ((0, 16), (1, 2)))
    return dict(tokens=tokens, norm_gain=norm_gain, gate_weight=gate_weight, up_weight=up_weight, down_weight=down_weight)


def reference(tokens, norm_gain, gate_weight, up_weight, down_weight):
    widened = tokens.astype(jnp.float32)
    squares = lax.optimization_barrier(jnp.sum(widened * widened, axis=1, keepdims=True))
    normed = (widened * norm_gain[None, :] / jnp.sqrt(squares / D + 1e-05)).astype(jnp.bfloat16)
    gate = jnp.dot(normed, gate_weight, preferred_element_type=jnp.float32)
    up = jnp.dot(normed, up_weight, preferred_element_type=jnp.float32)
    hidden = (jax.nn.silu(gate) * up).astype(jnp.bfloat16)
    return jnp.dot(hidden, down_weight, preferred_element_type=jnp.float32).astype(jnp.bfloat16)
```

```python
import functools

import jax
import jax.numpy as jnp
from jax import lax
from jax.experimental import pallas as pl
from jax.experimental.pallas import tpu as pltpu
from jax.sharding import PartitionSpec as P

CHUNKS = 2
F32 = jnp.float32
BF16 = jnp.bfloat16


def tile_of(width, wanted):
    return wanted if width % wanted == 0 else width


def in_kernel(parts, first, last, *refs):
    tokens, refs = refs[:parts], refs[parts:]
    gain, gate_w, up_w, refs = refs[0], refs[1], refs[2], refs[3:]
    if not first:
        gate_in, up_in, square_in, refs = refs[0], refs[1], refs[2], refs[3:]
    gate_out, up_out, square_out, refs = refs[0], refs[1], refs[2], refs[3:]
    if last:
        send_gate, send_up, refs = refs[0], refs[1], refs[2:]
    scaled = refs[0]

    @pl.when(pl.program_id(0) == 0)
    def _():
        start = 0
        for part in tokens:
            rows = part.shape[0]
            wide = part[...].astype(F32)
            scaled[pl.ds(start, rows), :] = (wide * gain[...]).astype(BF16)
            total = square_in[pl.ds(start, rows), :] if not first else None
            for lane in range(0, wide.shape[1], 128):
                slab = wide[:, lane : lane + 128]
                total = slab * slab if total is None else total + slab * slab
            square_out[pl.ds(start, rows), :] = total
            start += rows

    left = scaled[...]
    gate = jnp.dot(left, gate_w[...], preferred_element_type=F32)
    up = jnp.dot(left, up_w[...], preferred_element_type=F32)
    if not first:
        gate = gate + gate_in[...]
        up = up + up_in[...]
    gate_out[...] = gate
    up_out[...] = up
    if last:
        send_gate[...] = gate.astype(BF16)
        send_up[...] = up.astype(BF16)


def project_in(chunk, tokens, gain, gate_w, up_w, carried, last):
    rows = sum(part.shape[0] for part in tokens)
    depth = tokens[0].shape[1]
    width = gate_w.shape[1]
    tile = tile_of(width, 256)
    whole = lambda a: pl.BlockSpec(a.shape, lambda j: (0, 0))
    column = pl.BlockSpec((rows, tile), lambda j: (0, j))
    weight = pl.BlockSpec((depth, tile), lambda j: (chunk, j))
    first = carried is None
    in_specs = [whole(part) for part in tokens]
    in_specs += [pl.BlockSpec((1, depth), lambda j: (0, chunk)), weight, weight]
    args = list(tokens) + [gain, gate_w, up_w]
    aliases = {}
    square_spec = pl.BlockSpec((rows, 128), lambda j: (0, 0))
    if not first:
        in_specs += [column, column, square_spec]
        args += list(carried)
    outs = [jax.ShapeDtypeStruct((rows, width), F32)] * 2 + [jax.ShapeDtypeStruct((rows, 128), F32)]
    out_specs = [column, column, square_spec]
    if last:
        outs += [jax.ShapeDtypeStruct((rows, width), BF16)] * 2
        out_specs += [column, column]
    return pl.pallas_call(
        functools.partial(in_kernel, len(tokens), first, last),
        grid=(width // tile,),
        in_specs=in_specs,
        out_specs=out_specs,
        out_shape=outs,
        scratch_shapes=[pltpu.VMEM((rows, depth), BF16)],
        compiler_params=pltpu.CompilerParams(vmem_limit_bytes=(40 if rows > 512 else 24) * 2**20),
        cost_estimate=pl.CostEstimate(flops=4 * rows * depth * width, bytes_accessed=4 * depth * width, transcendentals=0),
        name="project_in",
    )(*args)


def hidden_kernel(features, gate, up, square, gate_far, up_far, square_far, out):
    squares = jnp.sum(square[...] + square_far[...], axis=1, keepdims=True)
    scale = lax.rsqrt(squares / features + 1e-05)
    g = (gate[...] + gate_far[...].astype(F32)) * scale
    u = (up[...] + up_far[...].astype(F32)) * scale
    out[...] = (g / (1.0 + jnp.exp(-g)) * u).astype(BF16)


def make_hidden(features, mine, far):
    rows, width = mine[0].shape
    tile = tile_of(width, 256)
    column = pl.BlockSpec((rows, tile), lambda j: (0, j))
    square = pl.BlockSpec((rows, 128), lambda j: (0, 0))
    return pl.pallas_call(
        functools.partial(hidden_kernel, features),
        grid=(width // tile,),
        in_specs=[column, column, square] * 2,
        out_specs=column,
        out_shape=jax.ShapeDtypeStruct((rows, width), BF16),
        compiler_params=pltpu.CompilerParams(vmem_limit_bytes=24 * 2**20),
        cost_estimate=pl.CostEstimate(flops=10 * rows * width, bytes_accessed=14 * rows * width, transcendentals=rows * width),
        name="make_hidden",
    )(*mine, *far)


def out_kernel(hidden, w0, w1, send0, keep0, send1, keep1):
    group = hidden.shape[0] // 4
    a = jnp.dot(hidden[...], w0[...], preferred_element_type=F32)
    keep0[:group] = a[:group]
    keep0[group:] = a[2 * group : 3 * group]
    send0[:group] = a[group : 2 * group].astype(BF16)
    send0[group:] = a[3 * group :].astype(BF16)
    b = jnp.dot(hidden[...], w1[...], preferred_element_type=F32)
    keep1[...] = b[: 2 * group]
    send1[...] = b[2 * group :].astype(BF16)


def project_out(chunk, chunks, hidden, down_w):
    rows, depth = hidden.shape
    half = down_w.shape[1] // chunks // 2
    tile = tile_of(half, 256)
    steps = half // tile
    piece = pl.BlockSpec((rows // 2, tile), lambda j: (0, j))
    shape = lambda dtype: jax.ShapeDtypeStruct((rows // 2, half), dtype)
    return pl.pallas_call(
        out_kernel,
        grid=(steps,),
        in_specs=[
            pl.BlockSpec((rows, depth), lambda j: (0, 0)),
            pl.BlockSpec((depth, tile), lambda j: (0, 2 * chunk * steps + j)),
            pl.BlockSpec((depth, tile), lambda j: (0, (2 * chunk + 1) * steps + j)),
        ],
        out_specs=[piece] * 4,
        out_shape=[shape(BF16), shape(F32), shape(BF16), shape(F32)],
        compiler_params=pltpu.CompilerParams(vmem_limit_bytes=24 * 2**20),
        cost_estimate=pl.CostEstimate(flops=4 * rows * depth * half, bytes_accessed=4 * depth * half, transcendentals=0),
        name="project_out",
    )(hidden, down_w, down_w)


def solution(mesh):
    n = mesh.shape["row"]
    rest = n // 4

    def hop(value, offset):
        return lax.ppermute(value, "row", [(i, i ^ offset) for i in range(n)])

    def swap(value):
        return lax.ppermute(value, "col", [(0, 1), (1, 0)])

    def gather(own):
        column = jnp.concatenate([own] + [hop(own, 4 * k) for k in range(1, rest)], axis=0)
        half = column.shape[0] // 2
        beside = hop(column, 1)
        above = hop(column, 2)
        return [column, beside, above, hop(beside[:half], 2), hop(above[half:], 1)]

    def scatter(send0, keep0, send1, keep1):
        group = keep0.shape[0] // 2
        own = group // rest
        sum0 = keep0 + hop(send0, 1).astype(F32)
        sum1 = keep1 + hop(send1, 2).astype(F32)
        column0 = sum0[:group] + hop(sum0[group:].astype(BF16), 2).astype(F32)
        column1 = sum1[:group] + hop(sum1[group:].astype(BF16), 1).astype(F32)
        column = jnp.concatenate([column0, column1], axis=1)
        total = column[:own]
        for k in range(1, rest):
            total = total + hop(column[k * own : (k + 1) * own].astype(BF16), 4 * k).astype(F32)
        return total.astype(BF16)

    def on_device(tokens, norm_gain, gate_weight, up_weight, down_weight):
        features = tokens.shape[1] * mesh.shape["col"]
        gain = norm_gain[None, :]
        depth = tokens.shape[1] // CHUNKS
        carried, sends = None, None
        for c in range(CHUNKS):
            parts = gather(tokens[:, c * depth : (c + 1) * depth])
            result = project_in(c, parts, gain, gate_weight, up_weight, carried, c == CHUNKS - 1)
            carried, sends = result[:3], result[3:]
        far = [swap(sends[0]), swap(sends[1]), swap(carried[2])]
        hidden = make_hidden(features, carried, far)
        outs = [scatter(*project_out(c, CHUNKS, hidden, down_weight)) for c in range(CHUNKS)]
        return jnp.concatenate(outs, axis=1)

    return jax.shard_map(
        on_device,
        mesh=mesh,
        in_specs=(P("row", "col"), P("col"), P("col", "row"), P("col", "row"), P("row", "col")),
        out_specs=P("row", "col"),
        check_vma=False,
    )
```

```python
import functools

import jax
import jax.numpy as jnp
from jax import lax
from jax.experimental import pallas as pl
from jax.experimental.pallas import tpu as pltpu
from jax.sharding import PartitionSpec as P


CHUNKS = 2
PIECES = 4
F32 = jnp.float32
BF16 = jnp.bfloat16
MIB = 2**20
VMEM = pl.BlockSpec(memory_space=pltpu.VMEM)
HBM = pl.BlockSpec(memory_space=pltpu.HBM)


def size(*arrays):
    return sum(a.size * a.dtype.itemsize for a in arrays)


def call(kernel, outs, args, specs, limit, flops, out_specs=None, scratch=(), **more):
    return pl.pallas_call(
        kernel,
        out_shape=outs,
        in_specs=specs,
        out_specs=[VMEM] * len(outs) if out_specs is None else out_specs,
        scratch_shapes=scratch,
        compiler_params=pltpu.CompilerParams(vmem_limit_bytes=limit),
        cost_estimate=pl.CostEstimate(flops=flops, bytes_accessed=size(*args), transcendentals=0),
        **more,
    )(*args)


def copy_kernel(plan, *refs):
    sources, outs = refs[: len(refs) - len(plan)], refs[len(refs) - len(plan) :]
    for out, pieces in zip(outs, plan):
        at = 0
        for source, start, rows, left, lanes in pieces:
            out[pl.ds(at, rows), :] = sources[source][pl.ds(start, rows), pl.ds(left, lanes)]
            at += rows


def rearrange(sources, plan):
    shapes = [(sum(piece[2] for piece in pieces), pieces[0][4]) for pieces in plan]
    outs = [jax.ShapeDtypeStruct(shape, sources[0].dtype) for shape in shapes]
    limit = MIB + size(*sources) + size(*outs)
    return call(functools.partial(copy_kernel, plan), outs, sources, [VMEM] * len(sources), limit, 10**10)


def fetch_start(source, left, out, sems):
    pieces = sems.shape[0]
    step = out.shape[0] // pieces
    copies = [
        pltpu.make_async_copy(
            source.at[pl.ds(k * step, step), pl.ds(left, out.shape[1])], out.at[pl.ds(k * step, step), :], sems.at[k]
        )
        for k in range(pieces)
    ]
    for copy in copies:
        copy.start()
    return copies


def in_kernel(parts, left, lanes, first, last, *refs):
    tokens, refs = refs[: len(parts)], refs[len(parts) :]
    gain, weights, refs = refs[0], refs[1:3], refs[3:]
    carried, refs = (None, refs) if first else (refs[:3], refs[3:])
    down_w, refs = (refs[0], refs[1:]) if last else (None, refs)
    totals, square_out, refs = refs[:2], refs[2], refs[3:]
    sends, refs = (refs[:2], refs[2:]) if last else (None, refs)
    copies = []
    if last:
        copies, refs = fetch_start(down_w, 0, refs[0], refs[2]), refs[1:]
    scaled = refs[0]
    start = 0
    for part, offset in zip(tokens, parts):
        rows = part.shape[0]
        wide = part[:, pl.ds(offset, lanes)].astype(F32)
        scaled[pl.ds(start, rows), :] = (wide * gain[:, pl.ds(left, lanes)]).astype(BF16)
        total = None if first else carried[2][pl.ds(start, rows), :]
        for lane in range(0, lanes, 128):
            slab = wide[:, lane : lane + 128]
            total = slab * slab if total is None else total + slab * slab
        square_out[pl.ds(start, rows), :] = total
        start += rows
    for i in range(2):
        value = jnp.dot(scaled[...], weights[i][pl.ds(left, lanes), :], preferred_element_type=F32)
        if not first:
            value = value + carried[i][...]
        totals[i][...] = value
        if last:
            sends[i][...] = value.astype(BF16)
    for copy in copies:
        copy.wait()


def project_in(left, lanes, tokens, parts, gain, gate_w, up_w, carried, down_w):
    last = down_w is not None
    rows = sum(part.shape[0] for part in tokens)
    width = gate_w.shape[1]
    first = carried is None
    args = list(tokens) + [gain, gate_w, up_w] + ([] if first else list(carried))
    outs = [jax.ShapeDtypeStruct((rows, width), F32)] * 2 + [jax.ShapeDtypeStruct((rows, 128), F32)]
    specs = [VMEM] * len(args)
    if last:
        outs += [jax.ShapeDtypeStruct((rows, width), BF16)] * 2
        outs += [jax.ShapeDtypeStruct((down_w.shape[0], down_w.shape[1] // CHUNKS), BF16)]
        args += [down_w]
        specs += [HBM]
    return call(
        functools.partial(in_kernel, parts, left, lanes, first, last),
        outs,
        args,
        specs,
        6 * MIB,
        4 * rows * lanes * width,
        scratch=[
            pltpu.VMEM((rows, lanes), BF16),
            pltpu.SemaphoreType.DMA((PIECES,)),
        ],
        input_output_aliases={} if first else {len(tokens) + 3 + i: i for i in range(3)},
    )


def out_kernel(features, chunk, *refs):
    first = features is not None
    if first:
        (gate, up, square, gate_far, up_far, square_far), refs = refs[:6], refs[6:]
        near, down_w, hidden, refs = refs[0], refs[1], refs[2], refs[3:]
    else:
        (hidden, near), refs = refs[:2], refs[2:]
    send0, keep0, send1, keep1 = refs[:4]
    copies = []
    if first:
        copies = fetch_start(down_w, (chunk + 1) * near.shape[1], refs[4], refs[5])
        width = gate.shape[1]
        squares = jnp.sum(square[...] + square_far[...], axis=1, keepdims=True)
        scale = lax.rsqrt(squares / features + 1e-05)
        tile = 256 if width % 256 == 0 else width
        for lane in range(0, width, tile):
            at = pl.ds(lane, tile)
            g = (gate[:, at] + gate_far[:, at].astype(F32)) * scale
            u = (up[:, at] + up_far[:, at].astype(F32)) * scale
            hidden[:, at] = (g / (1.0 + jnp.exp(-g)) * u).astype(BF16)
    group = hidden.shape[0] // 4
    half = near.shape[1] // 2
    a = jnp.dot(hidden[...], near[:, pl.ds(0, half)], preferred_element_type=F32)
    keep0[:group] = a[:group]
    keep0[group:] = a[2 * group : 3 * group]
    send0[:group] = a[group : 2 * group].astype(BF16)
    send0[group:] = a[3 * group :].astype(BF16)
    b = jnp.dot(hidden[...], near[:, pl.ds(half, half)], preferred_element_type=F32)
    keep1[...] = b[: 2 * group]
    send1[...] = b[2 * group :].astype(BF16)
    for copy in copies:
        copy.wait()


def project_out(features, chunk, args, near, down_w):
    first = down_w is not None
    rows, depth = args[0].shape
    half = near.shape[1] // 2
    shape = lambda dtype: jax.ShapeDtypeStruct((rows // 2, half), dtype)
    outs = [shape(BF16), shape(F32), shape(BF16), shape(F32)]
    args = [*args, near]
    specs = [VMEM] * len(args)
    if first:
        args, specs = args + [down_w], specs + [HBM]
        outs = [jax.ShapeDtypeStruct((rows, depth), BF16)] + outs + [jax.ShapeDtypeStruct(near.shape, BF16)]
    return call(
        functools.partial(out_kernel, features if first else None, chunk),
        outs,
        args,
        specs,
        16 * MIB,
        4 * rows * depth * half,
        scratch=[pltpu.SemaphoreType.DMA((PIECES,))] if first else [],
    )


def solution(mesh):
    n = mesh.shape["row"]
    rest = n // 4

    def hop(value, offset):
        return lax.ppermute(value, "row", [(i, i ^ offset) for i in range(n)])

    def swap(value):
        return lax.ppermute(value, "col", [(0, 1), (1, 0)])

    def scatter(send0, keep0, send1, keep1):
        group = keep0.shape[0] // 2
        own = group // rest
        sum0 = keep0 + hop(send0, 1).astype(F32)
        sum1 = keep1 + hop(send1, 2).astype(F32)
        column0 = sum0[:group] + hop(sum0[group:].astype(BF16), 2).astype(F32)
        column1 = sum1[:group] + hop(sum1[group:].astype(BF16), 1).astype(F32)
        column = jnp.concatenate([column0, column1], axis=1)
        total = column[:own]
        for k in range(1, rest):
            total = total + hop(column[k * own : (k + 1) * own].astype(BF16), 4 * k).astype(F32)
        return total.astype(BF16)

    def on_device(tokens, norm_gain, gate_weight, up_weight, down_weight):
        features = tokens.shape[1] * mesh.shape["col"]
        gain = norm_gain[None, :]
        rows = tokens.shape[0]
        lanes = tokens.shape[1] // CHUNKS
        down_weight = pltpu.with_memory_space_constraint(down_weight, pltpu.HBM)
        mine = rearrange([tokens], [[(0, 0, rows, c * lanes, lanes)] for c in range(CHUNKS)])
        beside, above = hop(tokens, 1), hop(tokens, 2)
        columns = [[hop(mine[c], 4 * k) for k in range(1, rest)] for c in range(CHUNKS)]
        last0 = rearrange([beside], [[(0, 0, rows, 0, lanes)]])[0]
        last1 = rearrange([above], [[(0, 0, rows, lanes, lanes)]])[0]
        corner = [hop(last0, 2), hop(last1, 1)]
        carried, sends = None, None
        for c in range(CHUNKS):
            column = rearrange(columns[c], [[(k, 0, rows, 0, lanes) for k in range(rest - 1)]])[0]
            half = column.shape[0] // 2
            x, y = hop(column, 1), hop(column, 2)
            first, second = rearrange([x, y], [[(0, 0, half, 0, lanes)], [(1, half, half, 0, lanes)]])
            fy, fx = hop(first, 2), hop(second, 1)
            parts = [tokens, column, beside, x, above, y, corner[c], fy, fx]
            offsets = [c * lanes, 0, c * lanes, 0, c * lanes, 0, 0, 0, 0]
            result = project_in(c * lanes, lanes, parts, offsets, gain, gate_weight, up_weight, carried, down_weight if c == CHUNKS - 1 else None)
            carried, sends = result[:3], result[3:]
        far = [swap(sends[0]), swap(sends[1]), swap(carried[2])]
        hidden, *pieces, after = project_out(features, 0, [*carried, *far], sends[2], down_weight)
        outs = [scatter(*pieces), scatter(*project_out(None, 1, [hidden], after, None))]
        return jnp.concatenate(outs, axis=1)

    return jax.shard_map(
        on_device,
        mesh=mesh,
        in_specs=(P("row", "col"), P("col"), P("col", "row"), P("col", "row"), P("row", "col")),
        out_specs=P("row", "col"),
        check_vma=False,
    )
```

```python
import functools

import jax
import jax.numpy as jnp
from jax import lax
from jax.experimental import pallas as pl
from jax.experimental.pallas import tpu as pltpu
from jax.sharding import PartitionSpec as P


CHUNKS = 2
PIECES = 2
EARLY = 10**10
SHARES = (1, 1)
F32 = jnp.float32
BF16 = jnp.bfloat16
MIB = 2**20
VMEM = pl.BlockSpec(memory_space=pltpu.VMEM)
HBM = pl.BlockSpec(memory_space=pltpu.HBM)


def size(*arrays):
    return sum(a.size * a.dtype.itemsize for a in arrays)


def call(kernel, outs, args, specs, limit, flops, out_specs=None, scratch=(), **more):
    return pl.pallas_call(
        kernel,
        out_shape=outs,
        in_specs=specs,
        out_specs=[VMEM] * len(outs) if out_specs is None else out_specs,
        scratch_shapes=scratch,
        compiler_params=pltpu.CompilerParams(vmem_limit_bytes=limit),
        cost_estimate=pl.CostEstimate(flops=flops, bytes_accessed=size(*args), transcendentals=0),
        **more,
    )(*args)


def copy_kernel(plan, *refs):
    sources, outs = refs[: len(refs) - len(plan)], refs[len(refs) - len(plan) :]
    for out, pieces in zip(outs, plan):
        at = 0
        for source, start, rows, left, lanes in pieces:
            out[pl.ds(at, rows), :] = sources[source][pl.ds(start, rows), pl.ds(left, lanes)]
            at += rows


def rearrange(sources, plan, flops=10**6):
    shapes = [(sum(piece[2] for piece in pieces), pieces[0][4]) for pieces in plan]
    outs = [jax.ShapeDtypeStruct(shape, sources[0].dtype) for shape in shapes]
    limit = MIB + size(*sources) + size(*outs)
    return call(functools.partial(copy_kernel, plan), outs, sources, [VMEM] * len(sources), limit, flops)


def fetch_start(source, start, out, sems):
    pieces = sems.shape[0]
    step = out.shape[0] // pieces
    copies = [
        pltpu.make_async_copy(source.at[pl.ds(start + k * step, step), :], out.at[pl.ds(k * step, step), :], sems.at[k])
        for k in range(pieces)
    ]
    for copy in copies:
        copy.start()
    return copies


def fetch_kernel(start, source, out, sems):
    for copy in fetch_start(source, start, out, sems):
        copy.wait()


def fetch(source, start, rows):
    outs = [jax.ShapeDtypeStruct((rows, source.shape[1]), source.dtype)]
    sems = [pltpu.SemaphoreType.DMA((PIECES,))]
    return call(functools.partial(fetch_kernel, start), outs, [source], [HBM], MIB, 2 * 10**9, scratch=sems)[0]


def in_kernel(parts, left, lanes, first, last, *refs):
    tokens, refs = refs[: len(parts)], refs[len(parts) :]
    gain, weights, refs = refs[0], refs[1:3], refs[3:]
    carried, refs = (None, refs) if first else (refs[:3], refs[3:])
    totals, square_out, refs = refs[:2], refs[2], refs[3:]
    sends, refs = (refs[:2], refs[2:]) if last else (None, refs)
    scaled = refs[0]
    start = 0
    for part, offset in zip(tokens, parts):
        rows = part.shape[0]
        wide = part[:, pl.ds(offset, lanes)].astype(F32)
        scaled[pl.ds(start, rows), :] = (wide * gain[:, pl.ds(left, lanes)]).astype(BF16)
        total = None if first else carried[2][pl.ds(start, rows), :]
        for lane in range(0, lanes, 128):
            slab = wide[:, lane : lane + 128]
            total = slab * slab if total is None else total + slab * slab
        square_out[pl.ds(start, rows), :] = total
        start += rows
    for i in range(2):
        value = jnp.dot(scaled[...], weights[i][pl.ds(left, lanes), :], preferred_element_type=F32)
        if not first:
            value = value + carried[i][...]
        totals[i][...] = value
        if last:
            sends[i][...] = value.astype(BF16)


def project_in(left, lanes, tokens, parts, gain, gate_w, up_w, carried, last):
    rows = sum(part.shape[0] for part in tokens)
    width = gate_w.shape[1]
    first = carried is None
    args = list(tokens) + [gain, gate_w, up_w] + ([] if first else list(carried))
    outs = [jax.ShapeDtypeStruct((rows, width), F32)] * 2 + [jax.ShapeDtypeStruct((rows, 128), F32)]
    specs = [VMEM] * len(args)
    if last:
        outs += [jax.ShapeDtypeStruct((rows, width), BF16)] * 2
    return call(
        functools.partial(in_kernel, parts, left, lanes, first, last),
        outs,
        args,
        specs,
        6 * MIB * max(1, rows // 256),
        4 * rows * lanes * width,
        scratch=[
            pltpu.VMEM((rows, lanes), BF16),
        ],
        input_output_aliases={} if first else {len(tokens) + 3 + i: i for i in range(3)},
    )


def out_kernel(features, left, *refs):
    first = features is not None
    if first:
        (gate, up, square, gate_far, up_far, square_far), refs = refs[:6], refs[6:]
    else:
        hidden, refs = refs[0], refs[1:]
    downs, refs = refs[:2], refs[2:]
    if first:
        hidden, refs = refs[0], refs[1:]
        width = gate.shape[1]
        squares = jnp.sum(square[...] + square_far[...], axis=1, keepdims=True)
        scale = lax.rsqrt(squares / features + 1e-05)
        tile = 256 if width % 256 == 0 else width
        for lane in range(0, width, tile):
            at = pl.ds(lane, tile)
            g = (gate[:, at] + gate_far[:, at].astype(F32)) * scale
            u = (up[:, at] + up_far[:, at].astype(F32)) * scale
            hidden[:, at] = (g / (1.0 + jnp.exp(-g)) * u).astype(BF16)
    group = hidden.shape[0] // 4
    half = refs[0].shape[1]
    split = downs[0].shape[0]
    for i, (stay, go) in enumerate((((0, 2), (1, 3)), ((0, 1), (2, 3)))):
        send, keep = refs[2 * i : 2 * i + 2]
        at = pl.ds(left + i * half, half)
        value = jnp.dot(hidden[:, pl.ds(0, split)], downs[0][:, at], preferred_element_type=F32)
        value += jnp.dot(hidden[:, pl.ds(split, hidden.shape[1] - split)], downs[1][:, at], preferred_element_type=F32)
        for k in range(2):
            rows = pl.ds(k * group, group)
            keep[rows, :] = value[stay[k] * group : (stay[k] + 1) * group]
            send[rows, :] = value[go[k] * group : (go[k] + 1) * group].astype(BF16)


def project_out(features, left, width, args, downs):
    first = features is not None
    rows, depth = args[0].shape
    half = width // 2
    shape = lambda dtype: jax.ShapeDtypeStruct((rows // 2, half), dtype)
    outs = [shape(BF16), shape(F32), shape(BF16), shape(F32)]
    if first:
        outs = [jax.ShapeDtypeStruct((rows, depth), BF16)] + outs
    args = [*args, *downs]
    return call(
        functools.partial(out_kernel, features, left),
        outs,
        args,
        [VMEM] * len(args),
        8 * MIB * max(1, rows // 256),
        4 * rows * depth * half,
    )


def solution(mesh):
    n = mesh.shape["row"]
    steps = [1 << b for b in reversed(range(2, n.bit_length() - 1))]

    offsets = [0]
    for step in steps:
        offsets += [offset ^ step for offset in offsets]

    def hop(value, offset):
        return lax.ppermute(value, "row", [(i, i ^ offset) for i in range(n)])

    def swap(value):
        return lax.ppermute(value, "col", [(0, 1), (1, 0)])

    def scatter(send0, keep0, send1, keep1):
        group = keep0.shape[0] // 2
        sum0 = keep0 + hop(send0, 1).astype(F32)
        sum1 = keep1 + hop(send1, 2).astype(F32)
        column0 = sum0[:group] + hop(sum0[group:].astype(BF16), 2).astype(F32)
        column1 = sum1[:group] + hop(sum1[group:].astype(BF16), 1).astype(F32)
        total = jnp.concatenate([column0, column1], axis=1)
        own = total.shape[0] // len(offsets)
        result = total[:own]
        for k, offset in enumerate(offsets):
            if k > 0:
                block = total[k * own : (k + 1) * own].astype(BF16)
                result = result + hop(block, offset).astype(F32)
        return result.astype(BF16)

    def on_device(tokens, norm_gain, gate_weight, up_weight, down_weight):
        features = tokens.shape[1] * mesh.shape["col"]
        gain = norm_gain[None, :]
        rows = tokens.shape[0]
        lanes = tokens.shape[1] // CHUNKS
        split = down_weight.shape[0] * 3 // 7 // 64 * 64
        widths = [tokens.shape[1] * share // sum(SHARES) for share in SHARES]
        down_weight = pltpu.with_memory_space_constraint(down_weight, pltpu.HBM)
        mine = rearrange([tokens], [[(0, 0, rows, c * lanes, lanes)] for c in range(CHUNKS)], EARLY)
        beside, above = hop(tokens, 1), hop(tokens, 2)
        columns = []
        for c in range(CHUNKS):
            held = [mine[c]]
            for offset in steps:
                sent = held[0]
                if len(held) > 1:
                    sent = rearrange(held, [[(k, 0, a.shape[0], 0, lanes) for k, a in enumerate(held)]], EARLY)[0]
                held.append(hop(sent, offset))
            columns.append(held[1:])
        last0 = rearrange([beside], [[(0, 0, rows, 0, lanes)]], EARLY)[0]
        last1 = rearrange([above], [[(0, 0, rows, lanes, lanes)]], EARLY)[0]
        corner = [hop(last0, 2), hop(last1, 1)]
        carried, sends = None, None
        for c in range(CHUNKS):
            column = rearrange(columns[c], [[(k, 0, a.shape[0], 0, lanes) for k, a in enumerate(columns[c])]], EARLY)[0]
            half = column.shape[0] // 2
            x, y = hop(column, 1), hop(column, 2)
            first, second = rearrange([x, y], [[(0, 0, half, 0, lanes)], [(1, half, half, 0, lanes)]])
            fy, fx = hop(first, 2), hop(second, 1)
            parts = [tokens, column, beside, x, above, y, corner[c], fy, fx]
            offsets = [c * lanes, 0, c * lanes, 0, c * lanes, 0, 0, 0, 0]
            result = project_in(c * lanes, lanes, parts, offsets, gain, gate_weight, up_weight, carried, c == CHUNKS - 1)
            carried, sends = result[:3], result[3:]
        far = [swap(sends[0]), swap(sends[1]), swap(carried[2])]
        downs = [fetch(down_weight, 0, split)]
        downs.append(fetch(down_weight, split, down_weight.shape[0] - split))
        hidden, outs, left = None, [], 0
        for c, width in enumerate(widths):
            given = [hidden] if c else [*carried, *far]
            result = project_out(None if c else features, left, width, given, downs)
            if c == 0:
                hidden, result = result[0], result[1:]
            outs.append(scatter(*result))
            left += width
        return jnp.concatenate(outs, axis=1)

    step = jax.shard_map(
        on_device,
        mesh=mesh,
        in_specs=(P("row", "col"), P("col"), P("col", "row"), P("col", "row"), P("row", "col")),
        out_specs=P("row", "col"),
        check_vma=False,
    )
    return step
```
